32 devices in a mesh: data: 2 (over x), seq: 16 (over z, y, core).
Axes of the slice: x: 2, y: 2, z: 4, core: 2. Of those that a mesh axis runs over, the one named last changes fastest.
Arguments:
- x: bfloat16 [65536, 4096], P(('data', 'seq')), parts along dimension 0
- idx: int32 [12288], P(('data', 'seq')), parts along dimension 0
- r: float32 [65536], P(('data', 'seq')), parts along dimension 0
- g1: float32 [4096], replicated
- g2: float32 [4096], replicated
- wq: bfloat16 [4096, 32, 128], replicated
- wk: bfloat16 [4096, 8, 128], replicated
- wv: bfloat16 [4096, 8, 128], replicated
- wo: bfloat16 [32, 128, 4096], replicated
- w1: bfloat16 [4096, 14336], replicated
- w3: bfloat16 [4096, 14336], replicated
- w2: bfloat16 [14336, 4096], replicated
Outputs:
- output: bfloat16 [65536, 4096], P(('data', 'seq')), parts along dimension 0
There are 2 independent parts. The reference program is written for one: setup_inputs(seed, part) draws one part's arguments, and reference() takes and returns one part's arrays. A program takes and returns all parts, laid end to end along the dimension named above; an argument that names none is the same for every part.
All inputs are finite; a program needn't handle non-finite values.
Results may differ from the reference program's by a relative error of at most 0.00478233.
Values are sent between devices in bfloat16 or wider.
A program may use at most 2 GiB of HBM per device.

```python
import jax
import jax.numpy as jnp
from jax import lax

SEQ = 16
D = 4096
HQ = 32
HKV = 8
DH = 128
FF = 14336
KDEV = 256
EXTRA = 128
CAP = KDEV + EXTRA
TL = 8 * KDEV
NTOK = SEQ * TL
NSEL = SEQ * KDEV
QB = min(128, KDEV)
EPS = 1e-5


def pick_rows(u, c):
    rk = jnp.argsort(jnp.argsort(u))
    pos = jnp.where(rk < c, jnp.arange(TL), TL)
    return jnp.sort(pos)[:CAP].astype(jnp.int32)


def setup_inputs(seed: int = 0, part: int = 0) -> dict:
    kp = jax.random.split(jax.random.fold_in(jax.random.key(seed), part), 8)
    kd = jax.random.split(jax.random.fold_in(jax.random.fold_in(jax.random.key(seed), part), 7), 5)
    kw = jax.random.split(jax.random.key(seed + 1), 9)
    t = jnp.arange(NTOK, dtype=jnp.float32) / NTOK
    freq = jnp.arange(1, 4, dtype=jnp.float32)
    phase = jax.random.uniform(kp[0], (3,), jnp.float32, 0.0, 6.283)
    coef = 0.8 * jnp.sin(6.283185 * t[:, None] * freq[None, :] + phase[None, :])
    dirs = jax.random.normal(kp[1], (3, D), jnp.float32)
    x = jnp.dot(coef, dirs) + jax.random.normal(kp[2], (NTOK, D), jnp.float32)
    w = max(SEQ // 4, 1)
    bmax = min(EXTRA, KDEV // w)
    b = jax.random.randint(kd[0], (), (3 * bmax) // 4, bmax + 1)
    s0 = jax.random.randint(kd[1], (), 0, SEQ - 2 * w + 1)
    sgn = jnp.where(jax.random.bernoulli(kd[2], 0.5), 1, -1)
    d = jnp.arange(SEQ) - s0
    over = ((d >= 0) & (d < w)).astype(jnp.int32)
    under = ((d >= w) & (d < 2 * w)).astype(jnp.int32)
    counts = KDEV + b * sgn * (over - under)
    centre = jax.random.randint(kd[3], (SEQ, 1), 0, TL, dtype=jnp.int32)
    noise_bits = (jax.random.bits(kd[4], (SEQ, TL), jnp.uint32) >> 13).astype(jnp.int32)
    local_pos = jnp.arange(TL, dtype=jnp.int32)[None, :]
    centre_dist = jnp.abs(local_pos - centre)
    pull_scale = (3 << 19) // TL
    order_score = noise_bits + pull_scale * centre_dist
    idx = jax.vmap(pick_rows)(order_score, counts).reshape(SEQ * CAP)
    r = jax.random.uniform(kp[6], (NTOK,), jnp.float32, 0.75, 2.0)
    sd = D ** -0.5
    g1 = jax.random.uniform(kw[0], (D,), jnp.float32, 0.5, 1.5)
    g2 = jax.random.uniform(kw[1], (D,), jnp.float32, 0.5, 1.5)
    wq = (1.5 * sd * jax.random.normal(kw[2], (D, HQ, DH), jnp.float32)).astype(jnp.bfloat16)
    wk = (1.5 * sd * jax.random.normal(kw[3], (D, HKV, DH), jnp.float32)).astype(jnp.bfloat16)
    wv = (sd * jax.random.normal(kw[4], (D, HKV, DH), jnp.float32)).astype(jnp.bfloat16)
    wo = ((HQ * DH) ** -0.5 * jax.random.normal(kw[5], (HQ, DH, D), jnp.float32)).astype(jnp.bfloat16)
    w1 = (sd * jax.random.normal(kw[6], (D, FF), jnp.float32)).astype(jnp.bfloat16)
    w3 = (sd * jax.random.normal(kw[7], (D, FF), jnp.float32)).astype(jnp.bfloat16)
    w2 = (FF ** -0.5 * jax.random.normal(kw[8], (FF, D), jnp.float32)).astype(jnp.bfloat16)
    return dict(x=x.astype(jnp.bfloat16), idx=idx, r=r, g1=g1, g2=g2, wq=wq, wk=wk, wv=wv,
                wo=wo, w1=w1, w3=w3, w2=w2)


def rms_norm(v, g):
    vf = v.astype(jnp.float32)
    inv = lax.rsqrt(jnp.mean(vf * vf, axis=-1, keepdims=True) + EPS)
    return (vf * inv * g).astype(jnp.bfloat16)


def reference(x, idx, r, g1, g2, wq, wk, wv, wo, w1, w3, w2):
    f32 = jnp.float32
    bf = jnp.bfloat16
    home = jnp.arange(SEQ * CAP) // CAP
    pos = jnp.where(idx < TL, home * TL + idx, NTOK)
    rows = jnp.sort(pos)[:NSEL]
    z = x[rows]
    n = rms_norm(z, g1)
    k = jnp.dot(n, wk.reshape(D, HKV * DH), preferred_element_type=f32).astype(bf).reshape(NSEL, HKV, DH)
    v = jnp.dot(n, wv.reshape(D, HKV * DH), preferred_element_type=f32).astype(bf).reshape(NSEL, HKV, DH)
    kf = k.astype(f32)
    vf = v.astype(f32)
    grp = HQ // HKV
    wq2 = wq.reshape(D, HQ * DH)
    wo2 = wo.reshape(HQ * DH, D)
    keyr = jnp.arange(NSEL)

    def blk(b):
        zb = lax.dynamic_slice_in_dim(z, b * QB, QB, 0)
        nb = lax.dynamic_slice_in_dim(n, b * QB, QB, 0)
        qb = jnp.dot(nb, wq2, preferred_element_type=f32).astype(bf).reshape(QB, HKV, grp, DH)
        s = jnp.einsum('qhgd,khd->hgqk', qb.astype(f32), kf) * (DH ** -0.5)
        qr = b * QB + jnp.arange(QB)
        s = jnp.where(keyr[None, :] <= qr[:, None], s, -jnp.inf)
        pr = jax.nn.softmax(s, axis=-1).astype(bf)
        o = jnp.einsum('hgqk,khd->qhgd', pr.astype(f32), vf).astype(bf).reshape(QB, HQ * DH)
        ha = jnp.dot(o, wo2, preferred_element_type=f32).astype(bf)
        a = (zb.astype(f32) + ha.astype(f32)).astype(bf)
        n2 = rms_norm(a, g2)
        hid = (jax.nn.silu(jnp.dot(n2, w1, preferred_element_type=f32))
               * jnp.dot(n2, w3, preferred_element_type=f32)).astype(bf)
        m = jnp.dot(hid, w2, preferred_element_type=f32)
        return (ha.astype(f32) + m).astype(bf)

    delta = lax.map(blk, jnp.arange(NSEL // QB)).reshape(NSEL, D)
    upd = (z.astype(f32) + r[rows][:, None] * delta.astype(f32)).astype(bf)
    return x.at[rows].set(upd)
```

```python
import functools

import jax
import jax.numpy as jnp
from jax import lax
from jax.experimental import pallas as pl
from jax.experimental.pallas import tpu as pltpu
from jax.sharding import PartitionSpec as P

EPS = 1e-5
CH = 64
LANE = 128
PADR = 16
F32 = jnp.float32
BF = jnp.bfloat16
VMEM = 60000 * 1024


def rms_norm(v, g):
    vf = v.astype(F32)
    inv = lax.rsqrt(jnp.mean(vf * vf, axis=-1, keepdims=True) + EPS)
    return (vf * inv * g).astype(BF)


def short_rows(cap):
    return cap - CH


def attn_kernel(narr, nsub, self_first, first, last, cap, grp, meta, q_ref, *refs):
    blocks = refs[:narr]
    rest = refs[narr:]
    if first:
        acc_in = ml_in = None
    else:
        acc_in, ml_in = rest[:2]
        rest = rest[2:]
    if last:
        o_ref = rest[0]
        acc, m_ref, l_ref = rest[1:]
    else:
        acc_out, ml_out = rest[:2]
        acc, m_ref, l_ref = rest[2:]
    nch = cap // CH
    rows = grp * CH
    brow = 2 * cap + PADR
    coef = (LANE ** -0.5) * 1.4426950408889634
    if first:
        acc[...] = jnp.zeros_like(acc)
        m_ref[...] = jnp.full_like(m_ref, -jnp.inf)
        l_ref[...] = jnp.zeros_like(l_ref)
    else:
        acc[...] = acc_in[0]
        m_ref[...] = jnp.broadcast_to(ml_in[0, :, 0:1], m_ref.shape)
        l_ref[...] = jnp.broadcast_to(ml_in[0, :, 64:65], l_ref.shape)
    cnt = meta[0]

    def chunk(i, k, v, bias, c0, causal):
        w = k.shape[0]
        qs = jnp.concatenate([q_ref[i * CH:(i + 1) * CH, h * LANE:(h + 1) * LANE] for h in range(grp)], axis=0)
        s = lax.dot_general(qs, k, (((1,), (1,)), ((), ())), preferred_element_type=F32)
        if causal:
            row = i * CH + lax.rem(lax.broadcasted_iota(jnp.int32, s.shape, 0), CH)
            col = c0 + lax.broadcasted_iota(jnp.int32, s.shape, 1)
            s = jnp.where(col <= row, s, -jnp.inf)
        else:
            s = s + bias
        rs = pl.ds(i * rows, rows)
        mo = m_ref[rs, :]
        mn = jnp.maximum(mo, jnp.max(s, axis=1, keepdims=True))
        mw = jnp.concatenate([mn] * (w // LANE), axis=1)
        p = jnp.exp2((s - mw) * coef)
        al = jnp.exp2((mo - mn) * coef)
        m_ref[rs, :] = mn
        l_ref[rs, :] = al * l_ref[rs, :] + jnp.sum(p, axis=1, keepdims=True)
        acc[rs, :] = al * acc[rs, :] + jnp.dot(p.astype(BF), v, preferred_element_type=F32)

    def sub(blk, base, causal):
        main = (cap // LANE - 1) * LANE
        parts = ((0, main), (main, LANE))
        for c0, w in parts:
            def go():
                k = blk[pl.ds(base + c0, w), :]
                v = blk[pl.ds(base + cap + c0, w), :]
                if causal:
                    bias = None
                else:
                    bias = jnp.concatenate(
                        [blk[pl.ds(base + 2 * cap, PADR), :].astype(F32)[c0 // LANE + j:c0 // LANE + j + 1, :]
                         for j in range(w // LANE)], axis=1)
                    bias = jnp.where(bias > 0.5, 0.0, -jnp.inf)
                for i in range(nch - 1):
                    if not causal or (i + 1) * CH > c0:
                        chunk(i, k, v, bias, c0, causal)

                @pl.when(cnt > short_rows(cap))
                def _():
                    chunk(nch - 1, k, v, bias, c0, causal)

            if c0 == 0:
                go()
            else:
                fl = blk[pl.ds(base + 2 * cap, PADR), :].astype(F32)[c0 // LANE:c0 // LANE + 1, :]
                pl.when(jnp.max(fl) > 0.5)(go)

    for a in range(narr):
        lo = 0
        if self_first and a == 0:
            sub(blocks[0], 0, True)
            lo = 1

        def body(t, _, a=a):
            @pl.when(meta[1 + a * nsub + t] > 0)
            def _():
                sub(blocks[a], pl.multiple_of(t * brow, PADR), False)
            return 0

        lax.fori_loop(lo, nsub, body, 0)

    if last:
        for i in range(nch):
            lv = l_ref[i * rows:(i + 1) * rows, :]
            ov = jnp.where(lv > 0.0, acc[i * rows:(i + 1) * rows, :] / lv, 0.0).astype(BF)
            for h in range(grp):
                o_ref[i * CH:(i + 1) * CH, h * LANE:(h + 1) * LANE] = ov[h * CH:(h + 1) * CH, :]
    else:
        acc_out[0] = acc[...]
        lane = lax.broadcasted_iota(jnp.int32, m_ref.shape, 1)
        ml_out[0] = jnp.where(lane < 64, m_ref[...], l_ref[...])


def attn_stage(meta, q, blocks, nsub, state, self_first, last):
    cap, qd = q.shape
    hkv = blocks[0].shape[1] // LANE
    grp = qd // LANE // hkv
    first = state is None
    st_rows = cap * grp
    st_spec = pl.BlockSpec((1, st_rows, LANE), lambda g, m: (g, 0, 0))
    in_specs = [pl.BlockSpec((cap, grp * LANE), lambda g, m: (0, g))]
    in_specs += [pl.BlockSpec((b.shape[0], LANE), lambda g, m: (0, g)) for b in blocks]
    args = [q, *blocks]
    aliases = {}
    if not first:
        in_specs += [st_spec, st_spec]
        args += list(state)
    st_shape = jax.ShapeDtypeStruct((hkv, st_rows, LANE), F32)
    if last:
        out_shape = jax.ShapeDtypeStruct((cap, qd), BF)
        out_specs = pl.BlockSpec((cap, grp * LANE), lambda g, m: (0, g))
    else:
        out_shape = (st_shape, st_shape)
        out_specs = (st_spec, st_spec)
        if not first:
            n = 1 + len(args)
            aliases = {n - 2: 0, n - 1: 1}
    nkeys = len(blocks) * nsub * cap
    return pl.pallas_call(
        functools.partial(attn_kernel, len(blocks), nsub, self_first, first, last, cap, grp),
        grid_spec=pltpu.PrefetchScalarGridSpec(
            num_scalar_prefetch=1, grid=(hkv,), in_specs=in_specs, out_specs=out_specs,
            scratch_shapes=[pltpu.VMEM((st_rows, LANE), F32)] * 3),
        out_shape=out_shape,
        input_output_aliases=aliases,
        compiler_params=pltpu.CompilerParams(vmem_limit_bytes=VMEM),
        cost_estimate=pl.CostEstimate(flops=8 * cap * qd * nkeys, bytes_accessed=40_000_000,
                                      transcendentals=cap * qd // LANE * nkeys),
        name=f"attn_{'first' if first else 'last' if last else 'mid'}",
    )(meta, *args)


def wo_kernel(cnt, o_ref, w_ref, out_ref):
    cap = o_ref.shape[0]
    m0 = short_rows(cap)

    @pl.when(cnt[0] <= m0)
    def _():
        out_ref[:m0, :] = jnp.dot(o_ref[:m0, :], w_ref[...], preferred_element_type=F32).astype(BF)
        out_ref[m0:, :] = jnp.zeros((cap - m0, out_ref.shape[1]), BF)

    @pl.when(cnt[0] > m0)
    def _():
        out_ref[...] = jnp.dot(o_ref[...], w_ref[...], preferred_element_type=F32).astype(BF)


def wo_call(cnt, o, w):
    cap, kd = o.shape
    nd = w.shape[1]
    nb = 512
    return pl.pallas_call(
        wo_kernel,
        grid_spec=pltpu.PrefetchScalarGridSpec(
            num_scalar_prefetch=1, grid=(nd // nb,),
            in_specs=[pl.BlockSpec((cap, kd), lambda j, c: (0, 0)), pl.BlockSpec((kd, nb), lambda j, c: (0, j))],
            out_specs=pl.BlockSpec((cap, nb), lambda j, c: (0, j))),
        out_shape=jax.ShapeDtypeStruct((cap, nd), BF),
        compiler_params=pltpu.CompilerParams(vmem_limit_bytes=VMEM),
        cost_estimate=pl.CostEstimate(flops=2 * cap * kd * nd, bytes_accessed=2 * kd * nd, transcendentals=0),
        name="wo",
    )(cnt, o, w)


def mlp_kernel(cnt, z_ref, h_ref, g_ref, w1_ref, w3_ref, w2_ref, out_ref, acc, n2):
    j = pl.program_id(0)
    cap, dm = z_ref.shape
    m0 = short_rows(cap)
    nb = 512 if dm % 512 == 0 else dm

    @pl.when(j == 0)
    def _():
        def norm(t, _):
            rs = pl.ds(pl.multiple_of(t * 16, 16), 16)
            a = (z_ref[rs, :].astype(F32) + h_ref[rs, :].astype(F32)).astype(BF).astype(F32)
            inv = lax.rsqrt(jnp.mean(a * a, axis=-1, keepdims=True) + EPS)
            n2[rs, :] = (a * inv * g_ref[...]).astype(BF)
            return 0
        lax.fori_loop(0, cap // 16, norm, 0)
        acc[...] = jnp.zeros_like(acc)

    def step(m):
        a = n2[:m, :]
        t1 = jnp.dot(a, w1_ref[...], preferred_element_type=F32)
        t3 = jnp.dot(a, w3_ref[...], preferred_element_type=F32)
        u = (t1 * (1.0 / (1.0 + jnp.exp(-t1))) * t3).astype(BF)
        for c in range(0, dm, nb):
            acc[:m, c:c + nb] += jnp.dot(u, w2_ref[:, c:c + nb], preferred_element_type=F32)

    @pl.when(cnt[0] <= m0)
    def _():
        step(m0)

    @pl.when(cnt[0] > m0)
    def _():
        step(cap)

    @pl.when(j == pl.num_programs(0) - 1)
    def _():
        def fin(t, _):
            rs = pl.ds(pl.multiple_of(t * 16, 16), 16)
            out_ref[rs, :] = (h_ref[rs, :].astype(F32) + acc[rs, :]).astype(BF)
            return 0
        lax.fori_loop(0, cap // 16, fin, 0)


def mlp_call(cnt, z, h, g2, w1, w3, w2):
    cap, dm = z.shape
    ff = w1.shape[1]
    fb = 512
    whole = lambda j, c: (0, 0)
    one = pl.Buffered(1)
    return pl.pallas_call(
        mlp_kernel,
        grid_spec=pltpu.PrefetchScalarGridSpec(
            num_scalar_prefetch=1, grid=(ff // fb,),
            in_specs=[pl.BlockSpec((cap, dm), whole, pipeline_mode=one),
                      pl.BlockSpec((cap, dm), whole, pipeline_mode=one),
                      pl.BlockSpec((1, dm), whole, pipeline_mode=one),
                      pl.BlockSpec((dm, fb), lambda j, c: (0, j)),
                      pl.BlockSpec((dm, fb), lambda j, c: (0, j)),
                      pl.BlockSpec((fb, dm), lambda j, c: (j, 0))],
            out_specs=pl.BlockSpec((cap, dm), whole, pipeline_mode=one),
            scratch_shapes=[pltpu.VMEM((cap, dm), F32), pltpu.VMEM((cap, dm), BF)]),
        out_shape=jax.ShapeDtypeStruct((cap, dm), BF),
        compiler_params=pltpu.CompilerParams(vmem_limit_bytes=VMEM),
        cost_estimate=pl.CostEstimate(flops=6 * cap * dm * ff, bytes_accessed=6 * dm * ff, transcendentals=cap * ff),
        name="mlp",
    )(cnt, z, h, g2.reshape(1, dm), w1, w3, w2)


def solution(mesh):
    nseq = mesh.shape['seq']
    nchip = nseq // 2
    ring = list(range(0, nchip, 2)) + list(range(nchip - 1, 0, -2))
    place = [ring.index(c) for c in range(nchip)]
    half = nchip // 2
    swap = [(i, i ^ 1) for i in range(nseq)]
    turn = ([(2 * ring[i], 2 * ring[(i + 1) % nchip]) for i in range(nchip)]
            + [(2 * ring[i] + 1, 2 * ring[(i - 1) % nchip] + 1) for i in range(nchip)])
    rowspec = P(('data', 'seq'))
    rep = P()

    def body(x, idx, r, g1, g2, wq, wk, wv, wo, w1, w3, w2):
        tl, dm = x.shape
        cap = idx.shape[0]
        hq, hkvv, dh = wq.shape[1], wk.shape[1], wq.shape[2]
        me = lax.axis_index('seq')
        core = lax.rem(me, 2)
        cnt = jnp.sum((idx < tl).astype(jnp.int32))
        cnt1 = cnt.reshape(1)
        tok = jnp.arange(tl)
        z = jnp.dot((idx[:, None] == tok[None, :]).astype(BF), x, preferred_element_type=F32).astype(BF)
        n = rms_norm(z, g1)
        k = jnp.dot(n, wk.reshape(dm, hkvv * dh), preferred_element_type=F32).astype(BF)
        v = jnp.dot(n, wv.reshape(dm, hkvv * dh), preferred_element_type=F32).astype(BF)
        live = (jnp.arange(PADR * LANE) < cnt).astype(BF).reshape(PADR, LANE)
        own = jnp.concatenate([k, v, jnp.tile(live, (1, hkvv))], axis=0)
        brow = own.shape[0]
        other = lax.ppermute(own, 'seq', swap)
        cur = jnp.concatenate([own, other], axis=0)
        q = jnp.dot(n, wq.reshape(dm, hq * dh), preferred_element_type=F32).astype(BF)

        ringa = jnp.array(ring, jnp.int32)
        pos = jnp.array(place, jnp.int32)[me // 2]

        def source(t):
            up = ringa[lax.rem(pos - t + nchip, nchip)]
            down = ringa[lax.rem(pos + t, nchip)]
            return jnp.where(core == 0, up, down), jnp.where(core == 0, down, up)

        def kind(dev):
            return (dev < me).astype(jnp.int32)

        def stage0():
            return attn_stage(jnp.stack([cnt, jnp.int32(1), kind(me ^ 1)]), q, [cur0], 2, None, True, False)

        cur0 = cur
        got = {}
        state = None
        for t in range(1, half + 1):
            fin = t == half
            mine = lax.ppermute(cur[:brow] if fin else cur, 'seq', turn)
            if t == 1:
                mine, q = lax.optimization_barrier((mine, q))
            else:
                state = stage0() if t == 2 else attn_stage(*got[t - 2], state, False, False)
                mine, state = lax.optimization_barrier((mine, state))
            his = lax.ppermute(mine, 'seq', swap)
            ca, cb = source(t)
            if fin:
                meta = [cnt, kind(2 * ca + core), kind(2 * cb + 1 - core)]
                nsub = 1
            else:
                meta = [cnt, kind(2 * ca + core), kind(2 * ca + 1 - core),
                        kind(2 * cb + 1 - core), kind(2 * cb + core)]
                nsub = 2
            got[t] = (jnp.stack(meta), q, [mine, his], nsub)
            cur = mine
        state = attn_stage(*got[half - 1], state, False, False)
        o = attn_stage(*got[half], state, False, True)
        h = wo_call(cnt1, o, wo.reshape(hq * dh, dm))
        delta = mlp_call(cnt1, z, h, g2, w1, w3, w2)
        dtok = jnp.dot((tok[:, None] == idx[None, :]).astype(BF), delta, preferred_element_type=F32)
        return (x.astype(F32) + r[:, None] * dtok).astype(BF)

    return jax.shard_map(body, mesh=mesh, in_specs=(rowspec, rowspec, rowspec) + (rep,) * 9,
                         out_specs=rowspec, check_vma=False)
```

```python
import functools

import jax
import jax.numpy as jnp
from jax import lax
from jax.experimental import pallas as pl
from jax.experimental.pallas import tpu as pltpu
from jax.sharding import PartitionSpec as P

EPS = 1e-5
CH = 32
TAIL = 64
LANE = 128
PADR = 16
TB = 128
F32 = jnp.float32
BF = jnp.bfloat16
VMEM = 60000 * 1024


def rms_norm(v, g):
    vf = v.astype(F32)
    inv = lax.rsqrt(jnp.mean(vf * vf, axis=-1, keepdims=True) + EPS)
    return (vf * inv * g).astype(BF)


def short_rows(cap):
    return cap - TAIL


def row_cases(cap):
    mid = short_rows(cap)
    low = mid // LANE * LANE
    return ((0, low), (low, mid), (mid, cap))


def attn_kernel(groups, first, last, cap, grp, ntail, narr, meta, q_ref, *refs):
    blocks = refs[:narr]
    rest = refs[narr:]
    if ntail:
        tail_ref, rest = rest[0], rest[1:]
    if first:
        x_ref, rest = rest[0], rest[1:]
        acc_in = ml_in = None
    else:
        acc_in, ml_in = rest[:2]
        rest = rest[2:]
    if last:
        o_ref = rest[0]
        acc, m_ref, l_ref = rest[1:]
    else:
        acc_out, ml_out = rest[:2]
        rest = rest[2:]
        if first:
            y_ref, rest = rest[0], rest[1:]
            y_ref[...] = x_ref[...]
        acc, m_ref, l_ref = rest
    nch = cap // CH
    rows = grp * CH
    mrow = short_rows(cap)
    main = mrow // LANE * LANE
    coef = (LANE ** -0.5) * 1.4426950408889634
    lane = lax.broadcasted_iota(jnp.int32, m_ref.shape, 1)
    if first:
        acc[...] = jnp.zeros_like(acc)
        m_ref[...] = jnp.full_like(m_ref, -jnp.inf)
        l_ref[...] = jnp.zeros_like(l_ref)
    else:
        acc[...] = acc_in[0]
        m_ref[...] = jnp.broadcast_to(ml_in[0, :, 0:1], m_ref.shape)
        l_ref[...] = jnp.where(lane == LANE - 1, ml_in[0], 0.0)
    cnt = meta[0]

    def chunk(i, k, v, bias, c0, causal):
        w = k.shape[0]
        qs = jnp.concatenate([q_ref[i * CH:(i + 1) * CH, h * LANE:(h + 1) * LANE] for h in range(grp)], axis=0)
        s = lax.dot_general(qs, k, (((1,), (1,)), ((), ())), preferred_element_type=F32)
        if causal:
            row = i * CH + lax.rem(lax.broadcasted_iota(jnp.int32, s.shape, 0), CH)
            col = c0 + lax.broadcasted_iota(jnp.int32, s.shape, 1)
            s = jnp.where(col <= row, s, -jnp.inf)
        else:
            s = s + bias
        rs = pl.ds(i * rows, rows)
        mo = m_ref[rs, :]
        mn = jnp.maximum(mo, jnp.max(s, axis=1, keepdims=True))
        mw = mn[:, :w] if w < LANE else jnp.concatenate([mn] * (w // LANE), axis=1)
        p = jnp.exp2((s - mw) * coef)
        al = jnp.exp2((mo - mn) * coef)
        m_ref[rs, :] = mn
        if w < LANE:
            ps = jnp.where(lane[:rows] == 0, jnp.sum(p, axis=1, keepdims=True), 0.0)
        else:
            ps = p[:, :LANE]
            for j in range(1, w // LANE):
                ps = ps + p[:, j * LANE:(j + 1) * LANE]
        l_ref[rs, :] = al * l_ref[rs, :] + ps
        acc[rs, :] = al * acc[rs, :] + jnp.dot(p.astype(BF), v, preferred_element_type=F32)

    def group(pieces, nrow, k0, causal):
        flags = [blk[pl.ds(base + 2 * nrow, PADR), :].astype(F32) for blk, base in pieces]
        head = nrow // LANE * LANE
        parts = [(0, head)] if head else []
        if nrow > head:
            parts.append((head, nrow - head))

        def part(c0, w):
            k = jnp.concatenate([blk[pl.ds(base + c0, w), :] for blk, base in pieces], axis=0)
            v = jnp.concatenate([blk[pl.ds(base + nrow + c0, w), :] for blk, base in pieces], axis=0)
            bias = None
            if not causal:
                row = c0 // LANE
                bias = jnp.concatenate([fl[row + j:row + j + 1, :min(w, LANE)]
                                        for fl in flags for j in range(-(-w // LANE))], axis=1)
                bias = jnp.where(bias > 0.5, 0.0, -jnp.inf)

            def run(lo, hi):
                for i in range(lo // CH, hi // CH):
                    if not causal or (i + 1) * CH > c0 + k0:
                        chunk(i, k, v, bias, c0 + k0, causal)

            run(0, main)

            @pl.when(cnt > main)
            def _():
                run(main, mrow)

            @pl.when(cnt > mrow)
            def _():
                run(mrow, cap)

        for c0, w in parts:
            if c0 == 0:
                part(c0, w)
            else:
                row = c0 // LANE
                some = flags[0][row:row + 1, :]
                for fl in flags[1:]:
                    some = jnp.maximum(some, fl[row:row + 1, :])

                @pl.when(jnp.max(some) > 0.5)
                def _():
                    part(c0, w)

    for n, (causal, pieces) in enumerate(groups):
        @pl.when(meta[1 + n] > 0)
        def _():
            group([(blocks[a], base) for a, base in pieces], mrow, 0, causal)

    if ntail:
        trow = 2 * TAIL + PADR

        def tail_body(t, _):
            base = pl.multiple_of(t * trow, PADR)
            for code, causal in ((1, False), (2, True)):
                @pl.when(meta[1 + len(groups) + t] == code)
                def _():
                    group([(tail_ref, base)], TAIL, mrow, causal)
            return 0

        lax.fori_loop(0, ntail, tail_body, 0)

    if last:
        for i in range(nch):
            lv = jnp.sum(l_ref[i * rows:(i + 1) * rows, :], axis=1, keepdims=True)
            ov = jnp.where(lv > 0.0, acc[i * rows:(i + 1) * rows, :] / lv, 0.0).astype(BF)
            for h in range(grp):
                o_ref[i * CH:(i + 1) * CH, h * LANE:(h + 1) * LANE] = ov[h * CH:(h + 1) * CH, :]
    else:
        acc_out[0] = acc[...]
        ml_out[0] = jnp.where(lane == LANE - 1, jnp.sum(l_ref[...], axis=1, keepdims=True), m_ref[...])


def attn_stage(meta, q, blocks, groups, state, last, tail=None, x=None):
    cap, qd = q.shape
    hkv = blocks[0].shape[1] // LANE
    grp = qd // LANE // hkv
    first = state is None
    st_rows = cap * grp
    st_spec = pl.BlockSpec((1, st_rows, LANE), lambda g, m: (g, 0, 0))
    in_specs = [pl.BlockSpec((cap, grp * LANE), lambda g, m: (0, g))]
    in_specs += [pl.BlockSpec((b.shape[0], LANE), lambda g, m: (0, g)) for b in blocks]
    args = [q, *blocks]
    aliases = {}
    ntail = 0
    if tail is not None:
        ntail = tail.shape[0] // (2 * TAIL + PADR)
        in_specs.append(pl.BlockSpec((tail.shape[0], LANE), lambda g, m: (0, g)))
        args.append(tail)
    if first:
        xs = pl.BlockSpec((x.shape[0] // hkv, x.shape[1]), lambda g, m: (g, 0))
        in_specs.append(xs)
        args.append(x)
    if not first:
        in_specs += [st_spec, st_spec]
        args += list(state)
    st_shape = jax.ShapeDtypeStruct((hkv, st_rows, LANE), F32)
    if last:
        out_shape = jax.ShapeDtypeStruct((cap, qd), BF)
        out_specs = pl.BlockSpec((cap, grp * LANE), lambda g, m: (0, g))
    else:
        out_shape = (st_shape, st_shape)
        out_specs = (st_spec, st_spec)
        if first:
            out_shape += (jax.ShapeDtypeStruct(x.shape, x.dtype),)
            out_specs += (xs,)
        else:
            n = 1 + len(args)
            aliases = {n - 2: 0, n - 1: 1}
    nkeys = sum(len(p) for _, p in groups) * cap
    return pl.pallas_call(
        functools.partial(attn_kernel, groups, first, last, cap, grp, ntail, len(blocks)),
        grid_spec=pltpu.PrefetchScalarGridSpec(
            num_scalar_prefetch=1, grid=(hkv,), in_specs=in_specs, out_specs=out_specs,
            scratch_shapes=[pltpu.VMEM((st_rows, LANE), F32)] * 3),
        out_shape=out_shape,
        input_output_aliases=aliases,
        compiler_params=pltpu.CompilerParams(vmem_limit_bytes=VMEM),
        cost_estimate=pl.CostEstimate(flops=8 * cap * qd * nkeys, bytes_accessed=40_000_000,
                                      transcendentals=cap * qd // LANE * nkeys),
        name=f"attn_{'first' if first else 'last' if last else 'mid'}",
    )(meta, *args)


def wo_kernel(cnt, o_ref, w_ref, out_ref):
    cap = o_ref.shape[0]
    for lo, hi in row_cases(cap):
        @pl.when((cnt[0] > lo) & (cnt[0] <= hi))
        def _():
            out_ref[:hi, :] = jnp.dot(o_ref[:hi, :], w_ref[...], preferred_element_type=F32).astype(BF)
            if hi < cap:
                out_ref[hi:, :] = jnp.zeros((cap - hi, out_ref.shape[1]), BF)


def wo_call(cnt, o, w):
    cap, kd = o.shape
    nd = w.shape[1]
    nb = 512
    return pl.pallas_call(
        wo_kernel,
        grid_spec=pltpu.PrefetchScalarGridSpec(
            num_scalar_prefetch=1, grid=(nd // nb,),
            in_specs=[pl.BlockSpec((cap, kd), lambda j, c: (0, 0)), pl.BlockSpec((kd, nb), lambda j, c: (0, j))],
            out_specs=pl.BlockSpec((cap, nb), lambda j, c: (0, j))),
        out_shape=jax.ShapeDtypeStruct((cap, nd), BF),
        compiler_params=pltpu.CompilerParams(vmem_limit_bytes=VMEM),
        cost_estimate=pl.CostEstimate(flops=2 * cap * kd * nd, bytes_accessed=2 * kd * nd, transcendentals=0),
        name="wo",
    )(cnt, o, w)


def mlp_kernel(cnt, z_ref, h_ref, g_ref, w1_ref, w3_ref, w2_ref, out_ref, acc, n2):
    j = pl.program_id(0)
    cap, dm = z_ref.shape
    nb = 512 if dm % 512 == 0 else dm

    @pl.when(j == 0)
    def _():
        def norm(t, _):
            rs = pl.ds(pl.multiple_of(t * 16, 16), 16)
            a = (z_ref[rs, :].astype(F32) + h_ref[rs, :].astype(F32)).astype(BF).astype(F32)
            inv = lax.rsqrt(jnp.mean(a * a, axis=-1, keepdims=True) + EPS)
            n2[rs, :] = (a * inv * g_ref[...]).astype(BF)
            return 0
        lax.fori_loop(0, cap // 16, norm, 0)
        acc[...] = jnp.zeros_like(acc)

    def step(m):
        a = n2[:m, :]
        t1 = jnp.dot(a, w1_ref[...], preferred_element_type=F32)
        t3 = jnp.dot(a, w3_ref[...], preferred_element_type=F32)
        u = (t1 * (1.0 / (1.0 + jnp.exp(-t1))) * t3).astype(BF)
        for c in range(0, dm, nb):
            acc[:m, c:c + nb] += jnp.dot(u, w2_ref[:, c:c + nb], preferred_element_type=F32)

    for lo, hi in row_cases(cap):
        @pl.when((cnt[0] > lo) & (cnt[0] <= hi))
        def _():
            step(hi)

    @pl.when(j == pl.num_programs(0) - 1)
    def _():
        def fin(t, _):
            rs = pl.ds(pl.multiple_of(t * 16, 16), 16)
            out_ref[rs, :] = (h_ref[rs, :].astype(F32) + acc[rs, :]).astype(BF)
            return 0
        lax.fori_loop(0, cap // 16, fin, 0)


def mlp_call(cnt, z, h, g2, w1, w3, w2):
    cap, dm = z.shape
    ff = w1.shape[1]
    fb = 512
    whole = lambda j, c: (0, 0)
    one = pl.Buffered(1)
    return pl.pallas_call(
        mlp_kernel,
        grid_spec=pltpu.PrefetchScalarGridSpec(
            num_scalar_prefetch=1, grid=(ff // fb,),
            in_specs=[pl.BlockSpec((cap, dm), whole, pipeline_mode=one),
                      pl.BlockSpec((cap, dm), whole, pipeline_mode=one),
                      pl.BlockSpec((1, dm), whole, pipeline_mode=one),
                      pl.BlockSpec((dm, fb), lambda j, c: (0, j)),
                      pl.BlockSpec((dm, fb), lambda j, c: (0, j)),
                      pl.BlockSpec((fb, dm), lambda j, c: (j, 0))],
            out_specs=pl.BlockSpec((cap, dm), whole, pipeline_mode=one),
            scratch_shapes=[pltpu.VMEM((cap, dm), F32), pltpu.VMEM((cap, dm), BF)]),
        out_shape=jax.ShapeDtypeStruct((cap, dm), BF),
        compiler_params=pltpu.CompilerParams(vmem_limit_bytes=VMEM),
        cost_estimate=pl.CostEstimate(flops=6 * cap * dm * ff, bytes_accessed=6 * dm * ff, transcendentals=cap * ff),
        name="mlp",
    )(cnt, z, h, g2.reshape(1, dm), w1, w3, w2)


def window(starts, b, cap):
    lo = jnp.minimum(starts[b] // 16 * 16, cap - TB - 16)
    return pl.ds(pl.multiple_of(lo, 16), TB + 16)


def touched(starts, b):
    return starts[b + 1] > starts[b]


def pick(idx_ref, win, b):
    ids = idx_ref[win, :]
    return (ids == b * TB + lax.broadcasted_iota(jnp.int32, ids.shape, 1)).astype(F32)


def gather_kernel(starts, x_any, idx_ref, g_ref, z_ref, n_ref, xbuf, zacc, sem):
    cap, dm = z_ref.shape
    nblk = xbuf.shape[0]
    nb = 512

    def copy(b):
        return pltpu.make_async_copy(x_any.at[pl.ds(pl.multiple_of(b * TB, TB), TB), :], xbuf.at[b], sem.at[b])

    def issue(b, _):
        @pl.when(touched(starts, b))
        def _():
            copy(b).start()
        return 0

    lax.fori_loop(0, nblk, issue, 0)
    zacc[...] = jnp.zeros_like(zacc)

    def step(b, _):
        @pl.when(touched(starts, b))
        def _():
            win = window(starts, b, cap)
            hot = pick(idx_ref, win, b).astype(BF)
            copy(b).wait()
            for c in range(0, dm, nb):
                zacc[win, c:c + nb] += jnp.dot(hot, xbuf[b, :, c:c + nb], preferred_element_type=F32)
        return 0

    lax.fori_loop(0, nblk, step, 0)

    def norm(t, _):
        rs = pl.ds(pl.multiple_of(t * 16, 16), 16)
        a = zacc[rs, :]
        inv = lax.rsqrt(jnp.mean(a * a, axis=-1, keepdims=True) + EPS)
        z_ref[rs, :] = a.astype(BF)
        n_ref[rs, :] = (a * inv * g_ref[...]).astype(BF)
        return 0

    lax.fori_loop(0, cap // 16, norm, 0)


def gather_call(starts, x, idxc, g1):
    tl, dm = x.shape
    cap = idxc.shape[0]
    nblk = tl // TB
    whole = lambda i, c: (0, 0)
    out = jax.ShapeDtypeStruct((cap, dm), BF)
    return pl.pallas_call(
        gather_kernel,
        grid_spec=pltpu.PrefetchScalarGridSpec(
            num_scalar_prefetch=1, grid=(1,),
            in_specs=[pl.BlockSpec(memory_space=pl.ANY), pl.BlockSpec((cap, LANE), whole), pl.BlockSpec((1, dm), whole)],
            out_specs=(pl.BlockSpec((cap, dm), whole),) * 2,
            scratch_shapes=[pltpu.VMEM((nblk, TB, dm), BF), pltpu.VMEM((cap, dm), F32),
                            pltpu.SemaphoreType.DMA((nblk,))]),
        out_shape=(out, out),
        compiler_params=pltpu.CompilerParams(vmem_limit_bytes=VMEM),
        cost_estimate=pl.CostEstimate(flops=2 * tl * cap * dm, bytes_accessed=2 * tl * dm, transcendentals=0),
        name="gather",
    )(starts, x, idxc, g1.reshape(1, dm))


def scatter_kernel(starts, y_in, d_ref, idx_ref, r_ref, y_any, ybuf, sem, osem):
    del y_in
    cap, dm = d_ref.shape
    nblk = ybuf.shape[0]
    nb = 512

    def rows(b):
        return y_any.at[pl.ds(pl.multiple_of(b * TB, TB), TB), :]

    def load(b):
        return pltpu.make_async_copy(rows(b), ybuf.at[b], sem.at[b])

    def save(b):
        return pltpu.make_async_copy(ybuf.at[b], rows(b), osem.at[b])

    def each(f):
        def go(b, _):
            @pl.when(touched(starts, b))
            def _():
                f(b)
            return 0
        lax.fori_loop(0, nblk, go, 0)

    def step(b):
        win = window(starts, b, cap)
        hot = pick(idx_ref, win, b).astype(BF)
        rv = r_ref[pl.ds(pl.multiple_of(b * TB, TB), TB), :]
        rv = jnp.concatenate([rv] * (nb // LANE), axis=1)
        load(b).wait()
        for c in range(0, dm, nb):
            d = lax.dot_general(hot, d_ref[win, c:c + nb], (((0,), (0,)), ((), ())), preferred_element_type=F32)
            ybuf[b, :, c:c + nb] = (ybuf[b, :, c:c + nb].astype(F32) + rv * d).astype(BF)
        save(b).start()

    each(lambda b: load(b).start())
    each(step)
    each(lambda b: save(b).wait())


def scatter_call(starts, y, delta, idxc, rc):
    tl, dm = y.shape
    cap = idxc.shape[0]
    nblk = tl // TB
    whole = lambda i, c: (0, 0)
    return pl.pallas_call(
        scatter_kernel,
        grid_spec=pltpu.PrefetchScalarGridSpec(
            num_scalar_prefetch=1, grid=(1,),
            in_specs=[pl.BlockSpec(memory_space=pl.ANY), pl.BlockSpec((cap, dm), whole),
                      pl.BlockSpec((cap, LANE), whole), pl.BlockSpec((tl, LANE), whole)],
            out_specs=pl.BlockSpec(memory_space=pl.ANY),
            scratch_shapes=[pltpu.VMEM((nblk, TB, dm), BF), pltpu.SemaphoreType.DMA((nblk,)),
                            pltpu.SemaphoreType.DMA((nblk,))]),
        out_shape=jax.ShapeDtypeStruct((tl, dm), BF),
        input_output_aliases={1: 0},
        compiler_params=pltpu.CompilerParams(vmem_limit_bytes=VMEM),
        cost_estimate=pl.CostEstimate(flops=2 * tl * cap * dm, bytes_accessed=4 * tl * dm, transcendentals=0),
        name="scatter",
    )(starts, y, delta, idxc, rc)


def solution(mesh):
    nseq = mesh.shape['seq']
    nchip = nseq // 2
    ring = list(range(0, nchip, 2)) + list(range(nchip - 1, 0, -2))
    place = [ring.index(c) for c in range(nchip)]
    half = nchip // 2
    swap = [(i, i ^ 1) for i in range(nseq)]
    turn = ([(2 * ring[i], 2 * ring[(i + 1) % nchip]) for i in range(nchip)]
            + [(2 * ring[i] + 1, 2 * ring[(i - 1) % nchip] + 1) for i in range(nchip)])
    rowspec = P(('data', 'seq'))
    rep = P()

    def body(x, idx, r, g1, g2, wq, wk, wv, wo, w1, w3, w2):
        tl, dm = x.shape
        cap = idx.shape[0]
        hq, hkvv, dh = wq.shape[1], wk.shape[1], wq.shape[2]
        me = lax.axis_index('seq')
        core = lax.rem(me, 2)
        cnt = jnp.sum((idx < tl).astype(jnp.int32))
        cnt1 = cnt.reshape(1)
        edges = jnp.arange(tl // TB + 1) * TB
        starts = jnp.sum((idx[None, :] < edges[:, None]).astype(jnp.int32), axis=1)
        idxc = jnp.broadcast_to(idx[:, None], (cap, LANE))
        rc = jnp.broadcast_to(r[:, None], (tl, LANE))
        z, n = gather_call(starts, x, idxc, g1)
        k = jnp.dot(n, wk.reshape(dm, hkvv * dh), preferred_element_type=F32).astype(BF)
        v = jnp.dot(n, wv.reshape(dm, hkvv * dh), preferred_element_type=F32).astype(BF)
        mrow = short_rows(cap)
        slot = jnp.arange(PADR * LANE)

        def pack(lo, hi):
            live = ((slot < hi - lo) & (slot + lo < cnt)).astype(BF).reshape(PADR, LANE)
            return jnp.concatenate([k[lo:hi], v[lo:hi], jnp.tile(live, (1, hkvv))], axis=0)

        own = pack(0, mrow)
        brow = own.shape[0]
        other = lax.ppermute(own, 'seq', swap)
        cur = jnp.concatenate([own, other], axis=0)
        q = jnp.dot(n, wq.reshape(dm, hq * dh), preferred_element_type=F32).astype(BF)

        ringa = jnp.array(ring, jnp.int32)
        pos = jnp.array(place, jnp.int32)[me // 2]

        def source(t):
            up = ringa[lax.rem(pos - t + nchip, nchip)]
            down = ringa[lax.rem(pos + t, nchip)]
            return jnp.where(core == 0, up, down), jnp.where(core == 0, down, up)

        def kind(dev):
            return (dev < me).astype(jnp.int32)

        def tails():
            most = lax.pmax(cnt, 'seq')
            shape = (nseq * (2 * TAIL + PADR), hkvv * dh)
            tail = lax.cond(most > mrow, lambda: lax.all_gather(pack(mrow, cap), 'seq', tiled=True),
                            lambda: jnp.zeros(shape, BF))
            dev = jnp.arange(nseq)
            kinds = jnp.where(dev < me, 1, jnp.where(dev == me, 2, 0)) * (most > mrow)
            return tail, kinds.astype(jnp.int32)

        def both(a):
            return (False, ((a, 0), (a, brow)))

        mine, his, kinds = {}, {}, {}
        cut = cur
        for t in range(1, half + 1):
            mine[t] = lax.ppermute(cut[:brow] if t == half else cut, 'seq', turn)
            if t == 1:
                mine[t], q = lax.optimization_barrier((mine[t], q))
            elif t == 3:
                tail, tkinds = tails()
                meta = jnp.concatenate([jnp.stack([cnt, jnp.int32(1), kind(me ^ 1), *kinds[1]]), tkinds])
                *state, y0 = attn_stage(meta, q, [cur, mine[1], his[1]],
                                        ((True, ((0, 0),)), (False, ((0, brow),)), both(1), both(2)),
                                        None, False, tail=tail, x=x)
                mine[t], state = lax.optimization_barrier((mine[t], state))
            his[t] = lax.ppermute(mine[t], 'seq', swap)
            ca, cb = source(t)
            kinds[t] = [kind(2 * ca), kind(2 * cb)]
            cut = mine[t]
        state = attn_stage(jnp.stack([cnt, *kinds[2]]), q, [mine[2], his[2]], (both(0), both(1)), state, False)
        o = attn_stage(jnp.stack([cnt, *kinds[3], kinds[4][0]]), q, [mine[3], his[3], mine[4], his[4]],
                       (both(0), both(1), (False, ((2, 0), (3, 0)))), state, True)
        h = wo_call(cnt1, o, wo.reshape(hq * dh, dm))
        delta = mlp_call(cnt1, z, h, g2, w1, w3, w2)
        return scatter_call(starts, y0, delta, idxc, rc)

    return jax.shard_map(body, mesh=mesh, in_specs=(rowspec, rowspec, rowspec) + (rep,) * 9,
                         out_specs=rowspec, check_vma=False)
```

```python
import functools

import jax
import jax.numpy as jnp
from jax import lax
from jax.experimental import pallas as pl
from jax.experimental.pallas import tpu as pltpu
from jax.sharding import PartitionSpec as P

EPS = 1e-5
CH = 64
LANE = 128
PADR = 16
TB = 128
F32 = jnp.float32
BF = jnp.bfloat16
VMEM = 60000 * 1024


def rms_norm(v, g):
    vf = v.astype(F32)
    inv = lax.rsqrt(jnp.mean(vf * vf, axis=-1, keepdims=True) + EPS)
    return (vf * inv * g).astype(BF)


def short_rows(cap):
    return cap - CH


def attn_kernel(subs, self_first, first, last, cap, grp, meta, q_ref, *refs):
    narr = len(subs)
    blocks = refs[:narr]
    rest = refs[narr:]
    if first:
        x_ref, rest = rest[0], rest[1:]
        acc_in = ml_in = None
    else:
        acc_in, ml_in = rest[:2]
        rest = rest[2:]
    if last:
        o_ref = rest[0]
        acc, m_ref, l_ref = rest[1:]
    else:
        acc_out, ml_out = rest[:2]
        rest = rest[2:]
        if first:
            y_ref, rest = rest[0], rest[1:]
            y_ref[...] = x_ref[...]
        acc, m_ref, l_ref = rest
    rows = grp * CH
    brow = 2 * cap + PADR
    mid = short_rows(cap)
    low = mid // LANE * LANE
    coef = (LANE ** -0.5) * 1.4426950408889634
    lane = lax.broadcasted_iota(jnp.int32, m_ref.shape, 1)
    if first:
        acc[...] = jnp.zeros_like(acc)
        m_ref[...] = jnp.full_like(m_ref, -jnp.inf)
        l_ref[...] = jnp.zeros_like(l_ref)
    else:
        acc[...] = acc_in[0]
        m_ref[...] = jnp.broadcast_to(ml_in[0, :, 0:1], m_ref.shape)
        l_ref[...] = jnp.where(lane == LANE - 1, ml_in[0], 0.0)
    cnt = meta[0]

    def chunk(i, k, v, bias, c0, causal):
        w = k.shape[0]
        qs = jnp.concatenate([q_ref[i * CH:(i + 1) * CH, h * LANE:(h + 1) * LANE] for h in range(grp)], axis=0)
        s = lax.dot_general(qs, k, (((1,), (1,)), ((), ())), preferred_element_type=F32)
        if causal:
            row = i * CH + lax.rem(lax.broadcasted_iota(jnp.int32, s.shape, 0), CH)
            col = c0 + lax.broadcasted_iota(jnp.int32, s.shape, 1)
            s = jnp.where(col <= row, s, -jnp.inf)
        else:
            s = s + bias
        rs = pl.ds(i * rows, rows)
        mo = m_ref[rs, :]
        mn = jnp.maximum(mo, jnp.max(s, axis=1, keepdims=True))
        p = jnp.exp2((s - jnp.concatenate([mn] * (w // LANE), axis=1)) * coef)
        al = jnp.exp2((mo - mn) * coef)
        m_ref[rs, :] = mn
        ps = p[:, :LANE]
        for j in range(1, w // LANE):
            ps = ps + p[:, j * LANE:(j + 1) * LANE]
        l_ref[rs, :] = al * l_ref[rs, :] + ps
        acc[rs, :] = al * acc[rs, :] + jnp.dot(p.astype(BF), v, preferred_element_type=F32)

    def sub(blk, base, causal):
        main = (cap // LANE - 1) * LANE

        def part(c0, w):
            k = blk[pl.ds(base + c0, w), :]
            v = blk[pl.ds(base + cap + c0, w), :]
            bias = None
            if not causal:
                fl = blk[pl.ds(base + 2 * cap, PADR), :].astype(F32)
                bias = jnp.concatenate([fl[c0 // LANE + j:c0 // LANE + j + 1, :] for j in range(w // LANE)], axis=1)
                bias = jnp.where(bias > 0.5, 0.0, -jnp.inf)

            def run(lo, hi):
                for i in range(lo // CH, hi // CH):
                    if not causal or (i + 1) * CH > c0:
                        chunk(i, k, v, bias, c0, causal)

            run(0, low)

            @pl.when(cnt > low)
            def _():
                run(low, mid)

            @pl.when(cnt > mid)
            def _():
                run(mid, cap)

        part(0, main)
        fl = blk[pl.ds(base + 2 * cap, PADR), :].astype(F32)[main // LANE:main // LANE + 1, :]

        @pl.when(jnp.max(fl) > 0.5)
        def _():
            part(main, LANE)

    n = 1
    for a in range(narr):
        lo = 0
        if self_first and a == 0:
            sub(blocks[0], 0, True)
            lo = 1

        def body(t, _, a=a, n=n):
            @pl.when(meta[n + t] > 0)
            def _():
                sub(blocks[a], pl.multiple_of(t * brow, PADR), False)
            return 0

        lax.fori_loop(lo, subs[a], body, 0)
        n += subs[a]

    if last:
        for i in range(cap // CH):
            lv = jnp.sum(l_ref[i * rows:(i + 1) * rows, :], axis=1, keepdims=True)
            ov = jnp.where(lv > 0.0, acc[i * rows:(i + 1) * rows, :] / lv, 0.0).astype(BF)
            for h in range(grp):
                o_ref[i * CH:(i + 1) * CH, h * LANE:(h + 1) * LANE] = ov[h * CH:(h + 1) * CH, :]
    else:
        acc_out[0] = acc[...]
        ml_out[0] = jnp.where(lane == LANE - 1, jnp.sum(l_ref[...], axis=1, keepdims=True), m_ref[...])


def attn_stage(meta, q, blocks, state, last, x=None):
    cap, qd = q.shape
    hkv = blocks[0].shape[1] // LANE
    grp = qd // LANE // hkv
    first = state is None
    st_rows = cap * grp
    st_spec = pl.BlockSpec((1, st_rows, LANE), lambda g, m: (g, 0, 0))
    in_specs = [pl.BlockSpec((cap, grp * LANE), lambda g, m: (0, g))]
    in_specs += [pl.BlockSpec((b.shape[0], LANE), lambda g, m: (0, g)) for b in blocks]
    args = [q, *blocks]
    aliases = {}
    if first:
        xs = pl.BlockSpec((x.shape[0] // hkv, x.shape[1]), lambda g, m: (g, 0))
        in_specs.append(xs)
        args.append(x)
    if not first:
        in_specs += [st_spec, st_spec]
        args += list(state)
    st_shape = jax.ShapeDtypeStruct((hkv, st_rows, LANE), F32)
    if last:
        out_shape = jax.ShapeDtypeStruct((cap, qd), BF)
        out_specs = pl.BlockSpec((cap, grp * LANE), lambda g, m: (0, g))
    else:
        out_shape = (st_shape, st_shape)
        out_specs = (st_spec, st_spec)
        if first:
            out_shape += (jax.ShapeDtypeStruct(x.shape, x.dtype),)
            out_specs += (xs,)
        else:
            n = 1 + len(args)
            aliases = {n - 2: 0, n - 1: 1}
    subs = tuple(b.shape[0] // (2 * cap + PADR) for b in blocks)
    nkeys = sum(subs) * cap
    return pl.pallas_call(
        functools.partial(attn_kernel, subs, first, first, last, cap, grp),
        grid_spec=pltpu.PrefetchScalarGridSpec(
            num_scalar_prefetch=1, grid=(hkv,), in_specs=in_specs, out_specs=out_specs,
            scratch_shapes=[pltpu.VMEM((st_rows, LANE), F32)] * 3),
        out_shape=out_shape,
        input_output_aliases=aliases,
        compiler_params=pltpu.CompilerParams(vmem_limit_bytes=VMEM),
        cost_estimate=pl.CostEstimate(flops=8 * cap * qd * nkeys, bytes_accessed=40_000_000,
                                      transcendentals=cap * qd // LANE * nkeys),
        name=f"attn_{'first' if first else 'last' if last else 'mid'}",
    )(meta, *args)


def wo_kernel(cnt, o_ref, w_ref, out_ref):
    cap = o_ref.shape[0]
    m0 = short_rows(cap)

    @pl.when(cnt[0] <= m0)
    def _():
        out_ref[:m0, :] = jnp.dot(o_ref[:m0, :], w_ref[...], preferred_element_type=F32).astype(BF)
        out_ref[m0:, :] = jnp.zeros((cap - m0, out_ref.shape[1]), BF)

    @pl.when(cnt[0] > m0)
    def _():
        out_ref[...] = jnp.dot(o_ref[...], w_ref[...], preferred_element_type=F32).astype(BF)


def wo_call(cnt, o, w):
    cap, kd = o.shape
    nd = w.shape[1]
    nb = 512
    return pl.pallas_call(
        wo_kernel,
        grid_spec=pltpu.PrefetchScalarGridSpec(
            num_scalar_prefetch=1, grid=(nd // nb,),
            in_specs=[pl.BlockSpec((cap, kd), lambda j, c: (0, 0)), pl.BlockSpec((kd, nb), lambda j, c: (0, j))],
            out_specs=pl.BlockSpec((cap, nb), lambda j, c: (0, j))),
        out_shape=jax.ShapeDtypeStruct((cap, nd), BF),
        compiler_params=pltpu.CompilerParams(vmem_limit_bytes=VMEM),
        cost_estimate=pl.CostEstimate(flops=2 * cap * kd * nd, bytes_accessed=2 * kd * nd, transcendentals=0),
        name="wo",
    )(cnt, o, w)


def mlp_kernel(cnt, z_ref, h_ref, g_ref, w1_ref, w3_ref, w2_ref, out_ref, acc, n2, u_ref):
    j = pl.program_id(0)
    last = pl.num_programs(0) - 1
    cap, dm = z_ref.shape
    nb = 512 if dm % 512 == 0 else dm

    @pl.when(j == 0)
    def _():
        def norm(t, _):
            rs = pl.ds(pl.multiple_of(t * 16, 16), 16)
            a = (z_ref[rs, :].astype(F32) + h_ref[rs, :].astype(F32)).astype(BF).astype(F32)
            inv = lax.rsqrt(jnp.mean(a * a, axis=-1, keepdims=True) + EPS)
            n2[rs, :] = (a * inv * g_ref[...]).astype(BF)
            return 0
        lax.fori_loop(0, cap // 16, norm, 0)
        acc[...] = jnp.zeros_like(acc)
        u_ref[...] = jnp.zeros_like(u_ref)

    def down(m, u):
        for c in range(0, dm, nb):
            acc[:m, c:c + nb] += jnp.dot(u, w2_ref[:, c:c + nb], preferred_element_type=F32)

    mid = short_rows(cap)
    for lo, hi in ((0, mid), (mid, cap)):
        mine = (cnt[0] > lo) & (cnt[0] <= hi)

        @pl.when(mine & (j < last))
        def _():
            a = n2[:hi, :]
            u = u_ref[:hi, :]
            t1 = jnp.dot(a, w1_ref[...], preferred_element_type=F32)
            t3 = jnp.dot(a, w3_ref[...], preferred_element_type=F32)
            down(hi, u)
            u_ref[:hi, :] = (t1 * (1.0 / (1.0 + jnp.exp(-t1))) * t3).astype(BF)

        @pl.when(mine & (j == last))
        def _():
            down(hi, u_ref[:hi, :])

    @pl.when(j == last)
    def _():
        def fin(t, _):
            rs = pl.ds(pl.multiple_of(t * 16, 16), 16)
            out_ref[rs, :] = (h_ref[rs, :].astype(F32) + acc[rs, :]).astype(BF)
            return 0
        lax.fori_loop(0, cap // 16, fin, 0)


def mlp_call(cnt, z, h, g2, w1, w3, w2):
    cap, dm = z.shape
    ff = w1.shape[1]
    fb = 512
    nff = ff // fb
    up = lambda j, c: (0, jnp.minimum(j, nff - 1))
    whole = lambda j, c: (0, 0)
    one = pl.Buffered(1)
    return pl.pallas_call(
        mlp_kernel,
        grid_spec=pltpu.PrefetchScalarGridSpec(
            num_scalar_prefetch=1, grid=(nff + 1,),
            in_specs=[pl.BlockSpec((cap, dm), whole, pipeline_mode=one),
                      pl.BlockSpec((cap, dm), whole, pipeline_mode=one),
                      pl.BlockSpec((1, dm), whole, pipeline_mode=one),
                      pl.BlockSpec((dm, fb), up), pl.BlockSpec((dm, fb), up),
                      pl.BlockSpec((fb, dm), lambda j, c: (jnp.maximum(j - 1, 0), 0))],
            out_specs=pl.BlockSpec((cap, dm), whole, pipeline_mode=one),
            scratch_shapes=[pltpu.VMEM((cap, dm), F32), pltpu.VMEM((cap, dm), BF), pltpu.VMEM((cap, fb), BF)]),
        out_shape=jax.ShapeDtypeStruct((cap, dm), BF),
        compiler_params=pltpu.CompilerParams(vmem_limit_bytes=VMEM),
        cost_estimate=pl.CostEstimate(flops=6 * cap * dm * ff, bytes_accessed=6 * dm * ff, transcendentals=cap * ff),
        name="mlp",
    )(cnt, z, h, g2.reshape(1, dm), w1, w3, w2)


def window(starts, b, cap):
    lo = jnp.minimum(starts[b] // 16 * 16, cap - TB - 16)
    return pl.ds(pl.multiple_of(lo, 16), TB + 16)


def touched(starts, b):
    return starts[b + 1] > starts[b]


def pick(idx_ref, win, b):
    ids = idx_ref[win, :]
    return (ids == b * TB + lax.broadcasted_iota(jnp.int32, ids.shape, 1)).astype(F32)


def scatter_kernel(starts, y_in, d_ref, idx_ref, r_ref, y_any, ybuf, sem, osem):
    del y_in
    cap, dm = d_ref.shape
    nblk = ybuf.shape[0]
    nb = 512

    def rows(b):
        return y_any.at[pl.ds(pl.multiple_of(b * TB, TB), TB), :]

    def load(b):
        return pltpu.make_async_copy(rows(b), ybuf.at[b], sem.at[b])

    def save(b):
        return pltpu.make_async_copy(ybuf.at[b], rows(b), osem.at[b])

    def each(f):
        def go(b, _):
            @pl.when(touched(starts, b))
            def _():
                f(b)
            return 0
        lax.fori_loop(0, nblk, go, 0)

    def step(b):
        win = window(starts, b, cap)
        hot = pick(idx_ref, win, b).astype(BF)
        rv = r_ref[pl.ds(pl.multiple_of(b * TB, TB), TB), :]
        rv = jnp.concatenate([rv] * (nb // LANE), axis=1)
        load(b).wait()
        for c in range(0, dm, nb):
            d = lax.dot_general(hot, d_ref[win, c:c + nb], (((0,), (0,)), ((), ())), preferred_element_type=F32)
            ybuf[b, :, c:c + nb] = (ybuf[b, :, c:c + nb].astype(F32) + rv * d).astype(BF)
        save(b).start()

    each(lambda b: load(b).start())
    each(step)
    each(lambda b: save(b).wait())


def scatter_call(starts, y, delta, idxc, rc):
    tl, dm = y.shape
    cap = idxc.shape[0]
    nblk = tl // TB
    whole = lambda i, c: (0, 0)
    return pl.pallas_call(
        scatter_kernel,
        grid_spec=pltpu.PrefetchScalarGridSpec(
            num_scalar_prefetch=1, grid=(1,),
            in_specs=[pl.BlockSpec(memory_space=pl.ANY), pl.BlockSpec((cap, dm), whole),
                      pl.BlockSpec((cap, LANE), whole), pl.BlockSpec((tl, LANE), whole)],
            out_specs=pl.BlockSpec(memory_space=pl.ANY),
            scratch_shapes=[pltpu.VMEM((nblk, TB, dm), BF), pltpu.SemaphoreType.DMA((nblk,)),
                            pltpu.SemaphoreType.DMA((nblk,))]),
        out_shape=jax.ShapeDtypeStruct((tl, dm), BF),
        input_output_aliases={1: 0},
        compiler_params=pltpu.CompilerParams(vmem_limit_bytes=VMEM),
        cost_estimate=pl.CostEstimate(flops=2 * tl * cap * dm, bytes_accessed=4 * tl * dm, transcendentals=0),
        name="scatter",
    )(starts, y, delta, idxc, rc)


def solution(mesh):
    nseq = mesh.shape['seq']
    nchip = nseq // 2
    ring = list(range(0, nchip, 2)) + list(range(nchip - 1, 0, -2))
    place = [ring.index(c) for c in range(nchip)]
    half = nchip // 2
    swap = [(i, i ^ 1) for i in range(nseq)]
    turn = ([(2 * ring[i], 2 * ring[(i + 1) % nchip]) for i in range(nchip)]
            + [(2 * ring[i] + 1, 2 * ring[(i - 1) % nchip] + 1) for i in range(nchip)])
    rowspec = P(('data', 'seq'))
    rep = P()

    def body(x, idx, r, g1, g2, wq, wk, wv, wo, w1, w3, w2):
        tl, dm = x.shape
        cap = idx.shape[0]
        hq, hkvv, dh = wq.shape[1], wk.shape[1], wq.shape[2]
        me = lax.axis_index('seq')
        core = lax.rem(me, 2)
        cnt = jnp.sum((idx < tl).astype(jnp.int32))
        cnt1 = cnt.reshape(1)
        tok = jnp.arange(tl)
        z = jnp.dot((idx[:, None] == tok[None, :]).astype(BF), x, preferred_element_type=F32).astype(BF)
        n = rms_norm(z, g1)
        k = jnp.dot(n, wk.reshape(dm, hkvv * dh), preferred_element_type=F32).astype(BF)
        v = jnp.dot(n, wv.reshape(dm, hkvv * dh), preferred_element_type=F32).astype(BF)
        live = (jnp.arange(PADR * LANE) < cnt).astype(BF).reshape(PADR, LANE)
        own = jnp.concatenate([k, v, jnp.tile(live, (1, hkvv))], axis=0)
        brow = own.shape[0]
        other = lax.ppermute(own, 'seq', swap)
        cur = jnp.concatenate([own, other], axis=0)
        q = jnp.dot(n, wq.reshape(dm, hq * dh), preferred_element_type=F32).astype(BF)

        ringa = jnp.array(ring, jnp.int32)
        pos = jnp.array(place, jnp.int32)[me // 2]

        def source(t):
            up = ringa[lax.rem(pos - t + nchip, nchip)]
            down = ringa[lax.rem(pos + t, nchip)]
            return jnp.where(core == 0, up, down), jnp.where(core == 0, down, up)

        def kind(dev):
            return (dev < me).astype(jnp.int32)

        mine, his, kinds = {}, {}, {}
        cut = cur
        for t in range(1, half + 1):
            mine[t] = lax.ppermute(cut[:brow] if t == half else cut, 'seq', turn)
            if t == 1:
                mine[t], q = lax.optimization_barrier((mine[t], q))
            else:
                if t == 2:
                    meta = jnp.stack([cnt, jnp.int32(1), kind(me ^ 1)])
                    *state, y0 = attn_stage(meta, q, [cur], None, False, x=x)
                else:
                    state = attn_stage(jnp.stack([cnt, *kinds[t - 2]]), q, [mine[t - 2], his[t - 2]], state, False)
                mine[t], state = lax.optimization_barrier((mine[t], state))
            his[t] = lax.ppermute(mine[t], 'seq', swap)
            ca, cb = source(t)
            ka, kb = kind(2 * ca), kind(2 * cb)
            kinds[t] = [ka, kb] if t == half else [ka, ka, kb, kb]
            cut = mine[t]
        t = half
        o = attn_stage(jnp.stack([cnt, *kinds[t - 1], *kinds[t]]), q, [mine[t - 1], his[t - 1], mine[t], his[t]],
                       state, True)
        h = wo_call(cnt1, o, wo.reshape(hq * dh, dm))
        delta = mlp_call(cnt1, z, h, g2, w1, w3, w2)
        edges = jnp.arange(tl // TB + 1) * TB
        starts = jnp.sum((idx[None, :] < edges[:, None]).astype(jnp.int32), axis=1)
        idxc = jnp.broadcast_to(idx[:, None], (cap, LANE))
        rc = jnp.broadcast_to(r[:, None], (tl, LANE))
        return scatter_call(starts, y0, delta, idxc, rc)

    return jax.shard_map(body, mesh=mesh, in_specs=(rowspec, rowspec, rowspec) + (rep,) * 9,
                         out_specs=rowspec, check_vma=False)
```
